256 devices in a mesh: batch: 16 (over z, y_hi), cols: 8 (over y_lo, x_hi, core), ens: 2 (over x_lo).
Axes of the slice: x: 4 (x_hi: 2, x_lo: 2; x = x_hi * 2 + x_lo), y: 4 (y_hi: 2, y_lo: 2; y = y_hi * 2 + y_lo), z: 8, core: 2. Of those that a mesh axis runs over, the one named last changes fastest.
Arguments:
- slope_up: float32 [32, 1280, 5120], P(('ens', 'batch'), None, 'cols'), parts along dimension 0, may hold values from -0.875 to 0.875
- slope_down: float32 [32, 5120, 1280], P(('ens', 'batch'), 'cols'), parts along dimension 0, may hold values from -0.875 to 0.875
- slope_norm: float32 [32, 1280], P(('ens', 'batch')), parts along dimension 0, may hold values from -8 to 8
- slope_bias: float32 [32, 1280], P(('ens', 'batch')), parts along dimension 0, may hold values from -8 to 8
- param_up: float32 [2560, 5120], P(('ens', 'batch'), 'cols'), parts along dimension 0, may hold values from -0.25 to 0.25
- param_down: float32 [10240, 1280], P(('ens', 'cols'), 'batch'), parts along dimension 0, may hold values from -0.125 to 0.125
- param_norm: float32 [2560], P(('ens', 'batch')), parts along dimension 0, may hold values from 0.25 to 1.75
- param_bias: float32 [2560], P(('ens', 'batch')), parts along dimension 0, may hold values from -3 to 3
Outputs:
- half_up: bfloat16 [2560, 5120], P('ens', 'cols'), parts along dimension 0
- half_down: bfloat16 [10240, 1280], P(('ens', 'cols')), parts along dimension 0
- half_norm: bfloat16 [2560], P('ens'), parts along dimension 0
- half_bias: bfloat16 [2560], P('ens'), parts along dimension 0
- next_up: float32 [2560, 5120], P(('ens', 'batch'), 'cols'), parts along dimension 0
- next_down: float32 [10240, 1280], P(('ens', 'cols'), 'batch'), parts along dimension 0
- next_norm: float32 [2560], P(('ens', 'batch')), parts along dimension 0
- next_bias: float32 [2560], P(('ens', 'batch')), parts along dimension 0
The draws below stay inside these ranges and needn't reach their ends.
There are 2 independent parts, one for each index of `ens`. The reference program is written for one: setup_inputs(seed, part) draws one part's arguments, and reference() takes and returns one part's arrays. A program takes and returns all parts, laid end to end along the dimension named above; each array names one. Nothing has to cross between parts.
All inputs are finite; a program needn't handle non-finite values.
Results may differ from the reference program's by a relative error of at most 0.008.
Values may be sent and summed in bfloat16 or wider, within the bound.
No kernel may reach another device: no remote copies, remote signals or barrier semaphores. Data moves between devices by JAX's collectives and lax.ppermute only.
A program may use at most 64 MiB of HBM per device.

```python
import jax
import jax.numpy as jnp
from jax import lax

WIDTH = 1280
INNER = 5120
REPLICAS = 16


def spiked(values, rng, source, target, shards_of, factor):
    owner, partner = [(jnp.arange(values.shape[position]) // (values.shape[position] // shards_of)).reshape([-1 if axis == position else 1 for axis in range(values.ndim)]) for position in (source, target)]
    chosen = jax.random.permutation(rng, shards_of)[partner]
    strong = (owner == chosen) | (owner == (partner + shards_of // 2) % shards_of)
    return jnp.where(strong, factor * values, values)


def block_levels(rng, dims, shards, low, high):
    loudness = 1.0
    for dim, blocks in shards:
        steps = jax.random.uniform(jax.random.fold_in(jax.random.fold_in(rng, 6), dim), (blocks,), jnp.float32, low / len(shards), high / len(shards))
        loudness = loudness * jnp.repeat(jnp.exp(steps), dims[dim] // blocks).reshape((-1,) + (1,) * (len(dims) - 1 - dim))
    return loudness


def bell_draw(key, dims, width, limit, shards=(), dtype=jnp.bfloat16):
    level = block_levels(key, dims, shards, -0.22, 0.18) if shards else 1.0
    drawn = jax.random.normal(key, dims, jnp.float32) * width * level
    return jnp.minimum(jnp.maximum(drawn, -limit), limit).astype(dtype)


def gaussian_with(key, extent, spread, most, shards, heavy, dtype=jnp.bfloat16):
    result = spread * jax.random.normal(key, extent, jnp.float32)
    if shards:
        result = result * block_levels(key, extent, shards, -0.22, 0.18)
    return jnp.clip(spiked(result, jax.random.fold_in(key, 3), *heavy), -most, most).astype(dtype)


def setup_inputs(seed: int = 0, part: int = 0) -> dict:
    streams_of = jax.random.split(jax.random.key(seed), 9)
    part_keys = jax.random.split(jax.random.fold_in(streams_of[8], part), 9)
    return {
        "slope_up": gaussian_with(part_keys[0], (REPLICAS, WIDTH, INNER), 0.1, 0.875, ((0, 16), (2, 8)), (0, 1, 16, 2.0), jnp.float32),
        "slope_down": gaussian_with(part_keys[1], (REPLICAS, INNER, WIDTH), 0.1, 0.875, ((0, 16), (1, 8)), (0, 2, 16, 2.0), jnp.float32),
        "slope_norm": gaussian_with(part_keys[2], (REPLICAS, WIDTH), 1.0, 8.0, ((0, 16),), (0, 1, 16, 2.0), jnp.float32),
        "slope_bias": gaussian_with(part_keys[3], (REPLICAS, WIDTH), 1.0, 8.0, ((0, 16),), (0, 1, 16, 2.0), jnp.float32),
        "param_up": gaussian_with(part_keys[4], (WIDTH, INNER), WIDTH ** -0.5, 0.25, ((0, 16), (1, 8)), (1, 0, 16, 2.0), jnp.float32),
        "param_down": gaussian_with(part_keys[5], (INNER, WIDTH), INNER ** -0.5, 0.125, ((0, 8), (1, 16)), (0, 1, 16, 2.0), jnp.float32),
        "param_norm": jnp.clip(1.0 + 0.15 * jax.random.normal(part_keys[6], (WIDTH,), jnp.float32), 0.25, 1.75),
        "param_bias": bell_draw(part_keys[7], (WIDTH,), 0.5, 3.0, ((0, 16),), jnp.float32),
    }


learn_rate = 0.4

def reference(slope_up, slope_down, slope_norm, slope_bias, param_up, param_down, param_norm, param_bias):
    mean_up = lax.optimization_barrier(jnp.sum(slope_up.astype(jnp.float32), axis=0)) * REPLICAS ** (-0.5)
    mean_down = lax.optimization_barrier(jnp.sum(slope_down.astype(jnp.float32), axis=0)) * REPLICAS ** (-0.5)
    mean_norm = lax.optimization_barrier(jnp.sum(slope_norm.astype(jnp.float32), axis=0)) * REPLICAS ** (-0.5)
    mean_bias = lax.optimization_barrier(jnp.sum(slope_bias.astype(jnp.float32), axis=0)) * REPLICAS ** (-0.5)
    ratio_up = jnp.sqrt(lax.optimization_barrier(jnp.sum(param_up * param_up, axis=1, keepdims=True))) * lax.rsqrt(lax.optimization_barrier(jnp.sum(mean_up * mean_up, axis=1, keepdims=True)) + 1e-06)
    mean_up = mean_up * ratio_up
    ratio_down = jnp.sqrt(lax.optimization_barrier(jnp.sum(param_down * param_down, axis=0, keepdims=True))) * lax.rsqrt(lax.optimization_barrier(jnp.sum(mean_down * mean_down, axis=0, keepdims=True)) + 1e-06)
    mean_down = mean_down * ratio_down
    next_up = param_up - learn_rate * mean_up
    next_down = param_down - learn_rate * mean_down
    next_norm = param_norm - learn_rate * mean_norm
    next_bias = param_bias - learn_rate * mean_bias
    half_up = next_up.astype(jnp.bfloat16)
    half_down = next_down.astype(jnp.bfloat16)
    half_norm = next_norm.astype(jnp.bfloat16)
    half_bias = next_bias.astype(jnp.bfloat16)
    return (half_up, half_down, half_norm, half_bias, next_up, next_down, next_norm, next_bias)
```

```python
import jax
import jax.numpy as jnp
from jax import lax
from jax.sharding import PartitionSpec as P

learn_rate = 0.4
f32, bf16 = jnp.float32, jnp.bfloat16


def ring(mesh_z, mesh_y, step):
    return [
        (z * mesh_y + h, (z + step) % mesh_z * mesh_y + h)
        for z in range(mesh_z)
        for h in range(mesh_y)
    ]


def xor(count, bit):
    return [(i, i ^ bit) for i in range(count)]


Z, Y = 8, 2


def forward(x):
    return lax.ppermute(x, "batch", ring(Z, Y, 1))


def backward(x):
    return lax.ppermute(x, "batch", ring(Z, Y, -1))


def across(x):
    return lax.ppermute(x, "batch", xor(Z * Y, 1))


def reduced(blocks):
    up = forward(blocks[4, 0])
    down = backward(blocks[4, 1])
    plus = jnp.stack([blocks[3, 0] + up, blocks[3, 1]])
    minus = jnp.stack([blocks[5, 0], blocks[5, 1] + down])
    for k in (2, 1):
        plus = forward(plus) + blocks[k]
        minus = backward(minus) + blocks[8 - k]
    plus, minus = forward(plus), backward(minus)
    total = plus.astype(f32) + minus.astype(f32) + blocks[0].astype(f32)
    other = across(total[1].astype(bf16))
    return total[0] + other.astype(f32)


def gathered(own):
    both = jnp.stack([own, across(own)])
    got = {0: both}
    plus = minus = both
    for k in (1, 2, 3):
        plus, minus = forward(plus), backward(minus)
        got[(8 - k) % 8], got[k] = plus, minus
    got[4] = jnp.stack([forward(plus[0]), backward(minus[1])])
    return jnp.stack([got[k] for k in range(8)])


def lane_sums(x):
    return (x * x).reshape(x.shape[0], -1, 128).sum(axis=1)


def over_cols(x):
    for bit in (1, 2, 4):
        x = x + lax.ppermute(x, "cols", xor(8, bit))
    return x.sum(axis=1, keepdims=True)


def on_device(
    slope_up, slope_down, slope_norm, slope_bias, param_up, param_down, param_norm, param_bias
):
    place = lax.axis_index("batch")
    z, y = place // Y, place % Y
    rel_z = (jnp.arange(8) + z) % 8
    rel_y = (jnp.arange(2) + y) % 2
    order = rel_z[:, None] * 2 + rel_y[None, :]

    def blocks_of(x):
        x = x.astype(bf16).reshape(16, 80, 640)
        return jnp.stack(
            [
                jnp.stack(
                    [lax.dynamic_index_in_dim(x, order[a, b], 0, keepdims=False) for b in range(2)]
                )
                for a in range(8)
            ]
        )

    vec = jnp.stack([slope_norm[0].reshape(16, 80), slope_bias[0].reshape(16, 80)], axis=1)
    vec = lax.all_to_all(vec.reshape(16, 1, 160), "batch", 0, 0, tiled=True).sum(axis=0)
    mean_norm, mean_bias = vec[0, :80] * 0.25, vec[0, 80:] * 0.25
    next_norm = param_norm - learn_rate * mean_norm
    next_bias = param_bias - learn_rate * mean_bias
    halves = jnp.concatenate([next_norm, next_bias]).astype(bf16)
    halves = jnp.broadcast_to(halves, (16, 1, 160))
    halves = lax.all_to_all(halves, "batch", 0, 0, tiled=True)
    half_norm = halves[:, 0, :80].reshape(-1)
    half_bias = halves[:, 0, 80:].reshape(-1)

    results = []
    for slope, param in ((slope_up[0], param_up), (slope_down[0].T, param_down.T)):
        own = over_cols(lane_sums(param))
        mean = reduced(blocks_of(slope)) * 0.25
        size = over_cols(lane_sums(mean))
        mean = mean * (jnp.sqrt(own) * lax.rsqrt(size + 1e-06))
        after = param - learn_rate * mean
        parts = gathered(after.astype(bf16))
        inverse_z = (jnp.arange(8) - z) % 8
        inverse_y = (jnp.arange(2) - y) % 2
        half = jnp.concatenate(
            [
                lax.dynamic_slice(parts, (inverse_z[a], inverse_y[b], 0, 0), (1, 1, 80, 640))[0, 0]
                for a in range(8)
                for b in range(2)
            ]
        )
        results.append((after, half))
    (next_up, half_up), (next_down, half_down) = results
    return (
        half_up,
        half_down.T,
        half_norm,
        half_bias,
        next_up,
        next_down.T,
        next_norm,
        next_bias,
    )


def solution(mesh):
    return jax.shard_map(
        on_device,
        mesh=mesh,
        in_specs=(
            P(("ens", "batch"), None, "cols"),
            P(("ens", "batch"), "cols", None),
            P(("ens", "batch"), None),
            P(("ens", "batch"), None),
            P(("ens", "batch"), "cols"),
            P(("ens", "cols"), "batch"),
            P(("ens", "batch")),
            P(("ens", "batch")),
        ),
        out_specs=(
            P("ens", "cols"),
            P(("ens", "cols"), None),
            P("ens"),
            P("ens"),
            P(("ens", "batch"), "cols"),
            P(("ens", "cols"), "batch"),
            P(("ens", "batch")),
            P(("ens", "batch")),
        ),
        check_vma=False,
    )
```

```python
import functools
import jax
import jax.numpy as jnp
from jax import lax
from jax.experimental import pallas as pl
from jax.experimental.pallas import tpu as pltpu
from jax.sharding import PartitionSpec as P

learn_rate = 0.4
mean_rate = 0.25
f32, bf16 = jnp.float32, jnp.bfloat16
Z, Y = 8, 2
ROWS, WIDE = 80, 640
SLAB = Y * ROWS
ALL = ROWS * 2 + 8
WINDOW = 256
VMEM = pl.BlockSpec(memory_space=pltpu.VMEM)
ANY = pl.BlockSpec(memory_space=pl.ANY)
SMEM = pl.BlockSpec(memory_space=pltpu.SMEM)


def ring(step):
    return [(z * Y + h, (z + step) % Z * Y + h) for z in range(Z) for h in range(Y)]


def xor(count, bit):
    return [(i, i ^ bit) for i in range(count)]


def forward(x):
    return lax.ppermute(x, "batch", ring(1))


def backward(x):
    return lax.ppermute(x, "batch", ring(-1))


def across(x, step=0):
    return lax.ppermute(x, "batch", [(a, b ^ 1) for a, b in ring(step)])


def slab_window(z):
    start = pl.multiple_of(z * SLAB // 128 * 128, 128)
    return start, pl.multiple_of(z * SLAB - start, 32)


def groups(shape, dim):
    place = lax.broadcasted_iota(jnp.int32, shape, dim)
    group = jnp.floor((place.astype(f32) + 0.5) * (1.0 / ROWS)).astype(jnp.int32)
    return group, place - group * ROWS


def rows_of(line):
    group, _ = groups((16, 16 * ROWS), 1)
    row = lax.broadcasted_iota(jnp.int32, (16, 16 * ROWS), 0)
    apart = jnp.where(group == row, line, 0.0).astype(bf16)
    _, within = groups((16 * ROWS, 128), 0)
    lane = lax.broadcasted_iota(jnp.int32, (16 * ROWS, 128), 1)
    return jnp.dot(apart, (within == lane).astype(bf16), preferred_element_type=f32)


def cut_body(shifts, norm, bias, up, down, *rest):
    n = len(shifts)
    outs, (wide, tall, turned, lines, sems) = rest[: 2 * n], rest[2 * n :]
    place = lax.axis_index("batch")
    y = place % Y
    places = [(place // Y + k) % Z for k in shifts]
    copies = []
    for i, z in enumerate(places):
        start, _ = slab_window(z)
        rows = pl.ds(pl.multiple_of(z * SLAB, SLAB), SLAB)
        copies.append(
            (
                pltpu.make_async_copy(down.at[:, pl.ds(start, WINDOW)], tall.at[i], sems.at[0, i]),
                pltpu.make_async_copy(up.at[rows], wide.at[i], sems.at[1, i]),
            )
        )
        for c in copies[-1]:
            c.start()
    lines[:16] = rows_of(norm[...])
    lines[16:] = rows_of(bias[...])
    for i, z in enumerate(places):
        _, shift = slab_window(z)
        copies[i][0].wait()
        turned[i] = tall[i].T.astype(bf16)
        copies[i][1].wait()
        for j, part in enumerate((1 - y, y)):
            out = outs[2 * i + j]
            from_up = pl.ds(pl.multiple_of(part * ROWS, ROWS), ROWS)
            from_down = pl.ds(pl.multiple_of(shift + part * ROWS, 16), ROWS)
            out[:ROWS] = wide[i, from_up].astype(bf16)
            out[ROWS : 2 * ROWS] = turned[i, from_down]
            row = z * Y + part
            line = jnp.concatenate(
                [
                    lines[pl.ds(row, 1), :],
                    lines[pl.ds(row + 16, 1), :],
                    jnp.zeros((1, WIDE - 256), f32),
                ],
                axis=1,
            )
            out[2 * ROWS :] = jnp.broadcast_to(line, (8, WIDE)).astype(bf16)


def cut(norm, bias, up, down, shifts):
    n = len(shifts)
    return pl.pallas_call(
        functools.partial(cut_body, shifts),
        out_shape=[pltpu.VMEM((ALL, WIDE), bf16)] * (2 * n),
        in_specs=[VMEM, VMEM, ANY, ANY],
        out_specs=[VMEM] * (2 * n),
        scratch_shapes=[
            pltpu.VMEM((n, SLAB, WIDE), f32),
            pltpu.VMEM((n, WIDE, WINDOW), f32),
            pltpu.VMEM((n, WINDOW, WIDE), bf16),
            pltpu.VMEM((32, 128), f32),
            pltpu.SemaphoreType.DMA((2, n)),
        ],
        name=f"cut_{n}",
    )(norm, bias, up, down)


def line_of(rows):
    group, within = groups((128, 16 * ROWS), 1)
    source = lax.broadcasted_iota(jnp.int32, (128, 16 * ROWS), 0)
    wide = jnp.dot(rows, (within == source).astype(bf16), preferred_element_type=f32)
    row = lax.broadcasted_iota(jnp.int32, (16, 16 * ROWS), 0)
    return jnp.sum(jnp.where(group[:16] == row, wide, 0.0), axis=0, keepdims=True)


def join_body(*rest):
    ins, (half_up, half_down, norm, bias) = rest[: 2 * Z], rest[2 * Z : 2 * Z + 4]
    whole, turned, lines, sems, sems_down = rest[2 * Z + 4 :]
    place = lax.axis_index("batch")
    y = place % Y
    copies = []
    for k in range(Z):
        z = (place // Y + k) % Z
        for j, part in enumerate((y, 1 - y)):
            src = ins[2 * k + j]
            at = pl.multiple_of((z * Y + part) * ROWS, 16)
            copies.append(
                pltpu.make_async_copy(
                    src.at[pl.ds(0, ROWS)], half_up.at[pl.ds(at, ROWS)], sems.at[2 * k + j]
                )
            )
            copies[-1].start()
            whole[pl.ds(at, ROWS), :] = src[ROWS : 2 * ROWS]
            lines[z * Y + part] = src[2 * ROWS :, :256].astype(f32)
    for c in range(10):
        turned[c] = whole[pl.ds(c * 128, 128), :].T
        copies.append(
            pltpu.make_async_copy(
                turned.at[c], half_down.at[:, pl.ds(c * 128, 128)], sems_down.at[c]
            )
        )
        copies[-1].start()
    first = lines[...][:, 0, :].astype(bf16)
    norm[...] = line_of(first[:, :128]).astype(bf16)
    bias[...] = line_of(first[:, 128:]).astype(bf16)
    for c in copies:
        c.wait()


def join(parts):
    return pl.pallas_call(
        join_body,
        out_shape=[
            jax.ShapeDtypeStruct((2 * Z * ROWS, WIDE), bf16),
            jax.ShapeDtypeStruct((WIDE, 2 * Z * ROWS), bf16),
            jax.ShapeDtypeStruct((1, 2 * Z * ROWS), bf16),
            jax.ShapeDtypeStruct((1, 2 * Z * ROWS), bf16),
        ],
        in_specs=[VMEM] * (2 * Z),
        out_specs=[ANY, ANY, VMEM, VMEM],
        scratch_shapes=[
            pltpu.VMEM((2 * Z * ROWS, WIDE), bf16),
            pltpu.VMEM((10, WIDE, 128), bf16),
            pltpu.VMEM((16, 8, 256), f32),
            pltpu.SemaphoreType.DMA((2 * Z,)),
            pltpu.SemaphoreType.DMA((10,)),
        ],
        name="join",
    )(*parts)


def summed(first, cut_more):
    other, own = dict(zip((4, 5, 3), first[::2])), dict(zip((4, 5, 3), first[1::2]))
    a_plus = forward(other[4])
    b_minus = backward(own[4])
    a_minus = backward(other[5])
    b_plus = forward(own[3])
    more = cut_more(a_plus)
    for i, k in enumerate((6, 2, 7, 1, 0)):
        other[k], own[k] = more[2 * i], more[2 * i + 1]
    near = across(other[0])
    a_plus = forward(a_plus + other[3])
    b_minus = backward(b_minus + own[5])
    a_minus = backward(a_minus + other[6])
    b_plus = forward(b_plus + own[2])
    a_plus = forward(a_plus + other[2])
    a_minus = across(a_minus + other[7], -1)
    b_minus = backward(b_minus + own[6])
    b_plus = forward(b_plus + own[1])
    a_plus = across(a_plus + other[1], 1)
    b_minus = backward(b_minus + own[7])
    total = b_plus.astype(f32) + a_minus.astype(f32) + (own[0].astype(f32) + near.astype(f32))
    return total + (a_plus.astype(f32) + b_minus.astype(f32))


def spread(a):
    a_plus, a_minus = forward(a), backward(a)
    b_plus, b_minus = across(a, 1), across(a, -1)
    got = {(0, 0): a, (0, 1): across(a)}
    for k in (1, 2, 3):
        if k > 1:
            a_plus, a_minus = forward(a_plus), backward(a_minus)
            b_plus, b_minus = forward(b_plus), backward(b_minus)
        got[8 - k, 0], got[k, 0], got[8 - k, 1], got[k, 1] = a_plus, a_minus, b_plus, b_minus
    got[4, 0], got[4, 1] = forward(a_plus), backward(b_minus)
    return [got[k, j] for k in range(Z) for j in range(Y)]


def squares(x):
    return jnp.sum(x * x, axis=1)


def over_cols(x):
    for bit in (1, 2, 4):
        x = x + lax.ppermute(x, "cols", xor(8, bit))
    return x


def vector_rows(norm, bias):
    n = norm.shape[0]
    line = jnp.concatenate([jnp.pad(norm, ((0, 0), (0, 48))), jnp.pad(bias, ((0, 0), (0, 48)))], 1)
    return jnp.pad(line.reshape(n, 1, 256), ((0, 0), (0, 7), (0, WIDE - 256)))


def on_device(
    slope_up, slope_down, slope_norm, slope_bias, param_up, param_down, param_norm, param_bias
):
    param = jnp.concatenate([param_up, param_down.T])
    args = (slope_norm, slope_bias, slope_up[0], slope_down[0])
    first = [*cut(*args, (4,)), *cut(*args, (5, 3))]

    def cut_more(after):
        norm, _ = lax.optimization_barrier((slope_norm, after))
        return cut(norm, *args[1:], (6, 2, 7, 1, 0))

    mean = summed(first, cut_more) * mean_rate
    vec, mean = mean[2 * ROWS], mean[: 2 * ROWS]
    next_norm = param_norm - learn_rate * vec[:ROWS]
    next_bias = param_bias - learn_rate * vec[128 : 128 + ROWS]
    sizes = over_cols(jnp.concatenate([squares(param), squares(mean)]))
    ratio = jnp.sqrt(sizes[: 2 * ROWS]) * lax.rsqrt(sizes[2 * ROWS :] + 1e-06)
    after = param - learn_rate * (mean * ratio[:, None])

    vec = vector_rows(next_norm[None], next_bias[None])[0]
    parts = spread(jnp.concatenate([after, vec]).astype(bf16))
    half_up, half_down, half_norm, half_bias = join(parts)
    return (
        half_up,
        half_down,
        half_norm.reshape(-1),
        half_bias.reshape(-1),
        after[:ROWS],
        after[ROWS:].T,
        next_norm,
        next_bias,
    )


def solution(mesh):
    return jax.shard_map(
        on_device,
        mesh=mesh,
        in_specs=(
            P(("ens", "batch"), None, "cols"),
            P(("ens", "batch"), "cols", None),
            P(("ens", "batch"), None),
            P(("ens", "batch"), None),
            P(("ens", "batch"), "cols"),
            P(("ens", "cols"), "batch"),
            P(("ens", "batch")),
            P(("ens", "batch")),
        ),
        out_specs=(
            P("ens", "cols"),
            P(("ens", "cols"), None),
            P("ens"),
            P("ens"),
            P(("ens", "batch"), "cols"),
            P(("ens", "cols"), "batch"),
            P(("ens", "batch")),
            P(("ens", "batch")),
        ),
        check_vma=False,
    )
```

```python
import functools
import jax
import jax.numpy as jnp
from jax import lax
from jax.experimental import pallas as pl
from jax.experimental.pallas import tpu as pltpu
from jax.sharding import PartitionSpec as P


learn_rate = 0.4
mean_rate = 0.25
f32, bf16 = jnp.float32, jnp.bfloat16
Z, Y = 8, 2
ROWS, WIDE = 80, 640
SLAB = Y * ROWS
ALL = ROWS * 2 + 8
GRANT = 12 << 20
EARLY = (0, 1, 7, 2, 6, 3, 5)
WINDOW = 256
VMEM = pl.BlockSpec(memory_space=pltpu.VMEM)
HBM = pl.BlockSpec(memory_space=pltpu.HBM)


def ring(step):
    return [(z * Y + h, (z + step) % Z * Y + h) for z in range(Z) for h in range(Y)]


def xor(count, bit):
    return [(i, i ^ bit) for i in range(count)]


def forward(x):
    return lax.ppermute(x, "batch", ring(1))


def backward(x):
    return lax.ppermute(x, "batch", ring(-1))


def across(x, step=0):
    return lax.ppermute(x, "batch", [(a, b ^ 1) for a, b in ring(step)])


def slab_window(z):
    start = pl.multiple_of(z * SLAB // 128 * 128, 128)
    return start, pl.multiple_of(z * SLAB - start, 32)


def groups(shape, dim):
    place = lax.broadcasted_iota(jnp.int32, shape, dim)
    group = jnp.floor((place.astype(f32) + 0.5) * (1.0 / ROWS)).astype(jnp.int32)
    return group, place - group * ROWS


def rows_of(line):
    group, _ = groups((16, 16 * ROWS), 1)
    row = lax.broadcasted_iota(jnp.int32, (16, 16 * ROWS), 0)
    apart = jnp.where(group == row, line, 0.0).astype(bf16)
    _, within = groups((16 * ROWS, 128), 0)
    lane = lax.broadcasted_iota(jnp.int32, (16 * ROWS, 128), 1)
    return jnp.dot(apart, (within == lane).astype(bf16), preferred_element_type=f32)


def cut_body(shifts, norm, bias, up, down, *rest):
    n = len(shifts)
    outs, (wide, tall, turned, lines, flat, sems, flat_sems) = rest[:-7], rest[-7:]
    place = lax.axis_index("batch")
    y = place % Y
    places = [(place // Y + k) % Z for k in shifts]
    vectors = [
        pltpu.make_async_copy(v, flat.at[i], flat_sems.at[i]) for i, v in enumerate((norm, bias))
    ]
    for c in vectors:
        c.start()
    copies = []
    for i, z in enumerate(places):
        start, _ = slab_window(z)
        rows = pl.ds(pl.multiple_of(z * SLAB, SLAB), SLAB)
        copies.append(
            (
                pltpu.make_async_copy(down.at[:, pl.ds(start, WINDOW)], tall.at[i], sems.at[0, i]),
                pltpu.make_async_copy(up.at[rows], wide.at[i], sems.at[1, i]),
            )
        )
        for c in copies[-1]:
            c.start()
    for c in vectors:
        c.wait()
    lines[:16] = rows_of(flat[0])
    lines[16:] = rows_of(flat[1])
    for i, z in enumerate(places):
        _, shift = slab_window(z)
        copies[i][0].wait()
        turned[i] = tall[i].T.astype(bf16)
        copies[i][1].wait()
        for j, part in enumerate((1 - y, y)):
            if len(outs) == 2 * n:
                out = outs[2 * i + j]
            else:
                out = outs[1 + i] if j else outs[0].at[pl.ds(i * ALL, ALL)]
            from_up = pl.ds(pl.multiple_of(part * ROWS, ROWS), ROWS)
            from_down = pl.ds(pl.multiple_of(shift + part * ROWS, 16), ROWS)
            out[:ROWS] = wide[i, from_up].astype(bf16)
            out[ROWS : 2 * ROWS] = turned[i, from_down]
            row = z * Y + part
            line = jnp.concatenate(
                [
                    lines[pl.ds(row, 1), :],
                    lines[pl.ds(row + 16, 1), :],
                    jnp.zeros((1, WIDE - 256), f32),
                ],
                axis=1,
            )
            out[2 * ROWS :] = jnp.broadcast_to(line, (8, WIDE)).astype(bf16)


def cut(norm, bias, up, down, shifts, joined=False):
    n = len(shifts)
    shapes = [pltpu.VMEM((ALL, WIDE), bf16)] * (n if joined else 2 * n)
    if joined:
        shapes = [pltpu.VMEM((n * ALL, WIDE), bf16)] + shapes
    return pl.pallas_call(
        functools.partial(cut_body, shifts),
        out_shape=shapes,
        in_specs=[HBM] * 4,
        out_specs=[VMEM] * len(shapes),
        scratch_shapes=[
            pltpu.VMEM((n, SLAB, WIDE), f32),
            pltpu.VMEM((n, WIDE, WINDOW), f32),
            pltpu.VMEM((n, WINDOW, WIDE), bf16),
            pltpu.VMEM((32, 128), f32),
            pltpu.VMEM((2, 1, 16 * ROWS), f32),
            pltpu.SemaphoreType.DMA((2, n)),
            pltpu.SemaphoreType.DMA((2,)),
        ],
        compiler_params=pltpu.CompilerParams(vmem_limit_bytes=GRANT),
    )(norm, bias, up, down)


def line_of(rows):
    group, within = groups((128, 16 * ROWS), 1)
    source = lax.broadcasted_iota(jnp.int32, (128, 16 * ROWS), 0)
    wide = jnp.dot(rows, (within == source).astype(bf16), preferred_element_type=f32)
    row = lax.broadcasted_iota(jnp.int32, (16, 16 * ROWS), 0)
    return jnp.sum(jnp.where(group[:16] == row, wide, 0.0), axis=0, keepdims=True)


def early_body(*rest):
    ins, (half_up, half_down, window, lines) = rest[: 2 * Z - 2], rest[2 * Z - 2 : 2 * Z + 2]
    whole, turned, sems, sems_down = rest[2 * Z + 2 :]
    place = lax.axis_index("batch")
    y = place % Y
    copies = []
    for i, k in enumerate(EARLY):
        z = (place // Y + k) % Z
        for j, part in enumerate((y, 1 - y)):
            src = ins[2 * i + j]
            at = pl.multiple_of((z * Y + part) * ROWS, 16)
            copies.append(
                pltpu.make_async_copy(
                    src.at[pl.ds(0, ROWS)], half_up.at[pl.ds(at, ROWS)], sems.at[2 * i + j]
                )
            )
            copies[-1].start()
            whole[pl.ds(at, ROWS), :] = src[ROWS : 2 * ROWS]
            lines[z * Y + part] = src[2 * ROWS :, :256].astype(f32)
    last = (place // Y + 4) % Z
    whole[pl.ds(pl.multiple_of(last * SLAB, SLAB), SLAB), :] = jnp.zeros((SLAB, WIDE), bf16)
    start, _ = slab_window(last)
    window[...] = whole[pl.ds(start, WINDOW), :]
    for c in range(10):
        turned[c] = whole[pl.ds(c * 128, 128), :].T
        copies.append(
            pltpu.make_async_copy(
                turned.at[c], half_down.at[:, pl.ds(c * 128, 128)], sems_down.at[c]
            )
        )
        copies[-1].start()
    for c in copies:
        c.wait()


def late_body(up_in, down_in, window, early_lines, own, other, half_up, half_down, norm, bias, *rest):
    whole, turned, lines, sems = rest
    place = lax.axis_index("batch")
    y = place % Y
    last = (place // Y + 4) % Z
    start, shift = slab_window(last)
    whole[...] = window[...]
    copies = []
    for j, (part, src) in enumerate(((y, own), (1 - y, other))):
        at = pl.multiple_of((last * Y + part) * ROWS, 16)
        copies.append(
            pltpu.make_async_copy(
                src.at[pl.ds(0, ROWS)], half_up.at[pl.ds(at, ROWS)], sems.at[j]
            )
        )
        copies[-1].start()
        whole[pl.ds(pl.multiple_of(shift + part * ROWS, 16), ROWS), :] = src[ROWS : 2 * ROWS]
    turned[...] = whole[...].T
    copies.append(pltpu.make_async_copy(turned, half_down.at[:, pl.ds(start, WINDOW)], sems.at[2]))
    copies[-1].start()
    lines[...] = early_lines[...]
    for part, src in ((y, own), (1 - y, other)):
        lines[last * Y + part] = src[2 * ROWS :, :256].astype(f32)
    first = lines[...][:, 0, :].astype(bf16)
    norm[...] = line_of(first[:, :128]).astype(bf16).reshape(2 * Z * ROWS)
    bias[...] = line_of(first[:, 128:]).astype(bf16).reshape(2 * Z * ROWS)
    for c in copies:
        c.wait()


def join(parts):
    up = jax.ShapeDtypeStruct((2 * Z * ROWS, WIDE), bf16)
    down = jax.ShapeDtypeStruct((WIDE, 2 * Z * ROWS), bf16)
    line = jax.ShapeDtypeStruct((2 * Z * ROWS,), bf16)
    half_up, half_down, window, lines = pl.pallas_call(
        early_body,
        out_shape=[up, down, pltpu.VMEM((WINDOW, WIDE), bf16), pltpu.VMEM((16, 8, 256), f32)],
        in_specs=[VMEM] * (2 * Z - 2),
        out_specs=[HBM, HBM, VMEM, VMEM],
        scratch_shapes=[
            pltpu.VMEM((2 * Z * ROWS, WIDE), bf16),
            pltpu.VMEM((10, WIDE, 128), bf16),
            pltpu.SemaphoreType.DMA((2 * Z - 2,)),
            pltpu.SemaphoreType.DMA((10,)),
        ],
        name="join_early",
        compiler_params=pltpu.CompilerParams(vmem_limit_bytes=GRANT),
    )(*(parts[k, j] for k in EARLY for j in range(Y)))
    return pl.pallas_call(
        late_body,
        out_shape=[up, down, line, line],
        in_specs=[HBM, HBM, VMEM, VMEM, VMEM, VMEM],
        out_specs=[HBM, HBM, VMEM, VMEM],
        input_output_aliases={0: 0, 1: 1},
        scratch_shapes=[
            pltpu.VMEM((WINDOW, WIDE), bf16),
            pltpu.VMEM((WIDE, WINDOW), bf16),
            pltpu.VMEM((16, 8, 256), f32),
            pltpu.SemaphoreType.DMA((3,)),
        ],
        name="join_late",
        compiler_params=pltpu.CompilerParams(vmem_limit_bytes=GRANT),
    )(half_up, half_down, window, lines, parts[4, 0], parts[4, 1])


def summed(cut_some):
    other, own = {}, {}
    other[4], own[4] = cut_some((4,))
    a_plus = forward(other[4])
    b_minus = backward(own[4])
    other[5], own[5], other[3], own[3] = cut_some((5, 3))
    a_minus = backward(other[5])
    b_plus = forward(own[3])
    blocks = cut_some((6, 2, 7, 1, 0))
    for i, k in enumerate((6, 2, 7, 1, 0)):
        other[k], own[k] = blocks[2 * i], blocks[2 * i + 1]
    near = across(other[0])
    a_plus = forward(a_plus + other[3])
    b_minus = backward(b_minus + own[5])
    a_minus = backward(a_minus + other[6])
    b_plus = forward(b_plus + own[2])
    a_plus = forward(a_plus + other[2])
    a_minus = across(a_minus + other[7], -1)
    b_minus = backward(b_minus + own[6])
    b_plus = forward(b_plus + own[1])
    a_plus = across(a_plus + other[1], 1)
    b_minus = backward(b_minus + own[7])
    total = b_plus.astype(f32) + a_minus.astype(f32) + (own[0].astype(f32) + near.astype(f32))
    return total + (a_plus.astype(f32) + b_minus.astype(f32))


def spread(a):
    a_plus, a_minus = forward(a), backward(a)
    n = a.shape[0]
    got = {(0, 0): a, (7, 0): a_plus, (1, 0): a_minus}
    a_plus2, a_minus2 = forward(a_plus), backward(a_minus)
    b_plus, b_minus = across(a_plus, 1), across(a_minus, -1)
    got[0, 1] = across(a)
    near = across(jnp.concatenate([a_plus, a_minus]))
    got[7, 1], got[1, 1] = near[:n], near[n:]
    got[6, 0], got[2, 0], got[6, 1], got[2, 1] = a_plus2, a_minus2, b_plus, b_minus
    a_plus, a_minus = forward(a_plus2), backward(a_minus2)
    b_plus, b_minus = forward(b_plus), backward(b_minus)
    got[5, 0], got[3, 0], got[5, 1], got[3, 1] = a_plus, a_minus, b_plus, b_minus
    got[4, 0], got[4, 1] = forward(a_plus), backward(b_minus)
    return got


def squares(x):
    return jnp.sum(x * x, axis=1)


def over_cols(x):
    for bit in (1, 2, 4):
        x = x + lax.ppermute(x, "cols", xor(8, bit))
    return x


def vector_rows(norm, bias):
    n = norm.shape[0]
    line = jnp.concatenate([jnp.pad(norm, ((0, 0), (0, 48))), jnp.pad(bias, ((0, 0), (0, 48)))], 1)
    return jnp.pad(line.reshape(n, 1, 256), ((0, 0), (0, 7), (0, WIDE - 256)))


def on_device(
    slope_up, slope_down, slope_norm, slope_bias, param_up, param_down, param_norm, param_bias
):
    param = jnp.concatenate([param_up, param_down.T])
    args = (slope_norm, slope_bias, slope_up[0], slope_down[0])
    args = [pltpu.with_memory_space_constraint(x, pltpu.HBM) for x in args]
    mean = summed(functools.partial(cut, *args)) * mean_rate
    vec, mean = mean[2 * ROWS], mean[: 2 * ROWS]
    next_norm = param_norm - learn_rate * vec[:ROWS]
    next_bias = param_bias - learn_rate * vec[128 : 128 + ROWS]
    sizes = over_cols(jnp.concatenate([squares(param), squares(mean)]))
    ratio = jnp.sqrt(sizes[: 2 * ROWS]) * lax.rsqrt(sizes[2 * ROWS :] + 1e-06)
    after = param - learn_rate * (mean * ratio[:, None])

    vec = vector_rows(next_norm[None], next_bias[None])[0]
    parts = spread(jnp.concatenate([after, vec]).astype(bf16))
    after, parts[5, 0] = lax.optimization_barrier((after, parts[5, 0]))
    half_up, half_down, half_norm, half_bias = join(parts)
    return (
        half_up,
        half_down,
        half_norm,
        half_bias,
        after[:ROWS],
        after[ROWS:].T,
        next_norm,
        next_bias,
    )


def solution(mesh):
    return jax.shard_map(
        on_device,
        mesh=mesh,
        in_specs=(
            P(("ens", "batch"), None, "cols"),
            P(("ens", "batch"), "cols", None),
            P(("ens", "batch"), None),
            P(("ens", "batch"), None),
            P(("ens", "batch"), "cols"),
            P(("ens", "cols"), "batch"),
            P(("ens", "batch")),
            P(("ens", "batch")),
        ),
        out_specs=(
            P("ens", "cols"),
            P(("ens", "cols"), None),
            P("ens"),
            P("ens"),
            P(("ens", "batch"), "cols"),
            P(("ens", "cols"), "batch"),
            P(("ens", "batch")),
            P(("ens", "batch")),
        ),
        check_vma=False,
    )
```
